512 devices in a mesh: parts: 2 (over y), blk: 128 (over z, x), merge: 2 (over core).
Axes of the slice: x: 4, y: 2, z: 32, core: 2. Of those that a mesh axis runs over, the one named last changes fastest.
The devices are a block of a 4x8x32 slice.
Arguments:
- queries: bfloat16 [2048, 1024], P('blk'), may hold values from -102 to 102
- spans: bfloat16 [65536, 1024], P(('parts', 'blk', 'merge')), parts along dimension 0, may hold values from -0.5 to 0.5
- span_doc: int32 [65536], P(('parts', 'blk', 'merge')), parts along dimension 0, may hold values from 0 to 127
- span_valid: int32 [65536], P(('parts', 'blk', 'merge')), parts along dimension 0, may hold values 0 or 1
- doc_bias: float32 [128], replicated, may hold values from -3 to 0
Outputs:
- soft_match: float32 [4096], P(('parts', 'blk')), parts along dimension 0
- top_score: float32 [4096], P(('parts', 'blk')), parts along dimension 0
The draws below stay inside these ranges and needn't reach their ends.
There are 2 independent parts, one for each index of `parts`. The reference program is written for one: setup_inputs(seed, part) draws one part's arguments, and reference() takes and returns one part's arrays. A program takes and returns all parts, laid end to end along the dimension named above; an argument that names none is the same for every part. Nothing has to cross between parts.
All inputs are finite; a program needn't handle non-finite values. No bound on the sum of `span_valid` on one device may be relied on, other than what follows from the above.
Results may differ from the reference program's by a relative error of at most 0.0003.
Values may be sent and summed in bfloat16 or wider, within the bound.
No kernel may reach another device: no remote copies, remote signals or barrier semaphores. Data moves between devices by JAX's collectives and lax.ppermute only.
A program may use at most 64 MiB of HBM per device.

```python
import jax
import jax.numpy as jnp
from jax import lax

E = 1024
DOCS = 128
NQ = 2048
NCH = 32768


def draw_queries(key, part):
    first = jax.random.fold_in(key, 0)
    base = jnp.clip(jax.random.normal(first, (NQ, E), jnp.float32), -6.0, 6.0)
    return base.astype(jnp.bfloat16)


def draw_spans(key, part):
    first = jax.random.fold_in(key, 0)
    third = jax.random.fold_in(key, 2)
    order = jax.random.permutation(third, NCH)
    rising = 0.5 + order.astype(jnp.float32) / NCH
    base = jnp.clip(jax.random.normal(first, (NCH, E), jnp.float32), -6.0, 6.0)
    values = base * rising[:, None] / jnp.sqrt(jnp.float32(E))
    return jnp.clip(values, -0.5, 0.5).astype(jnp.bfloat16)


def touch_ends(result, key, least, high):
    shape = result.shape
    place = [jax.random.randint(jax.random.fold_in(key, axis), (), 0, shape[axis]) for axis in range(len(shape))]
    result = result.at[tuple(place)].set(least)
    longest = shape.index(max(shape))
    place[longest] = (place[longest] + 1) % shape[longest]
    return result.at[tuple(place)].set(high)


def setup_inputs(seed: int = 0, part: int = 0) -> dict:
    key_of = jax.random.split(jax.random.key(seed), 6)
    part_splits = jax.random.split(jax.random.fold_in(key_of[5], part), 6)
    return {
        "queries": draw_queries(jax.random.fold_in(key_of[5], 71), part),
        "spans": draw_spans(jax.random.fold_in(jax.random.fold_in(key_of[5], part), 71), part),
        "span_doc": touch_ends(jax.random.randint(part_splits[2], (NCH,), 0, DOCS), jax.random.fold_in(part_splits[2], 1), 0, DOCS - 1).astype(jnp.int32),
        "span_valid": touch_ends((jax.random.randint(part_splits[3], (NCH,), 0, 8) < 7).astype(jnp.int32), jax.random.fold_in(part_splits[3], 1), 0, 1),
        "doc_bias": jnp.clip(jax.random.uniform(key_of[4], (DOCS,), jnp.float32, -3.0, 0.0), -3.0, 0.0),
    }


def span_bias(span_doc, doc_bias):
    onehot = span_doc[:, None] == jnp.arange(doc_bias.shape[0], dtype=jnp.int32)[None, :]
    return jnp.sum(jnp.where(onehot, doc_bias[None, :], jnp.zeros_like(doc_bias)[None, :]), axis=1)


def block_stats(rows, spans, bias, valid):
    similarity = lax.dot_general(rows, spans, (((1,), (1,)), ((), ())), preferred_element_type=jnp.float32)
    logit = jnp.where(valid[None, :], 2.0 * similarity + bias[None, :], -jnp.inf)
    highest = jnp.max(logit, axis=1)
    total = jnp.sum(jnp.exp(logit - highest[:, None]), axis=1)
    best = jnp.max(jnp.where(valid[None, :], similarity, -jnp.inf), axis=1)
    return highest, total, best


def reference(queries, spans, span_doc, span_valid, doc_bias):
    bias = span_bias(span_doc, doc_bias)
    valid = span_valid == 1
    blocks = queries.reshape(-1, 16, queries.shape[1])

    def one_block(rows):
        highest, total, best = block_stats(rows, spans, bias, valid)
        return highest + jnp.log(total), best

    soft, best = lax.map(one_block, blocks)
    return soft.reshape(-1), best.reshape(-1)
```

```python
import jax
import jax.numpy as jnp
from jax import lax
from jax.experimental import pallas as pl
from jax.experimental.pallas import tpu as pltpu
from jax.sharding import Mesh
from jax.sharding import PartitionSpec as P

RING = 32
ROW = 4
RESIDUES = 4
LOOP = RING // RESIDUES
FIRST = RING // 2
LOW = -1e30

GROUP = ("ring", "row", "merge")


def ring_place(residue, step):
    return (FIRST + RESIDUES * step + residue) % RING


def shifted(value, axis, by):
    size = lax.axis_size(axis)
    return lax.ppermute(value, axis, [(k, (k + by) % size) for k in range(size)])


def scores_kernel(shift_ref, bias_ref, *refs):
    packs, pieces, out_ref = refs[:8], refs[8:13], refs[13]
    rows_ref, sims_ref = refs[14:]
    rows = out_ref.shape[0] // 2
    at = 0
    for piece in pieces:
        size = piece.shape[0] * piece.shape[1]
        rows_ref[at : at + size, :] = piece[...].reshape(size, piece.shape[2])
        at += size
    count = packs[0].shape[0] - 8
    docs = lax.broadcasted_iota(jnp.int32, (count, bias_ref.shape[1]), 1).astype(jnp.float32)
    best = jnp.full((1, at), LOW, jnp.float32)
    biases = []
    for k, pack in enumerate(packs):
        code = pack[count:, :128].astype(jnp.float32).T[:, :1]
        bias = jnp.sum(jnp.where(docs == code, bias_ref[...], 0.0), axis=1, keepdims=True)
        valid = code < float(bias_ref.shape[1])
        biases.append(jnp.where(valid, bias, -jnp.inf))
        sim = lax.dot_general(
            pack[:count, :], rows_ref[...], (((1,), (1,)), ((), ())), preferred_element_type=jnp.float32
        )
        sims_ref[k] = sim
        best = jnp.maximum(best, jnp.max(jnp.where(valid, sim, LOW), axis=0, keepdims=True))
    total = jnp.zeros((1, at), jnp.float32)
    for k in range(len(packs)):
        total += jnp.sum(jnp.exp(2.0 * (sims_ref[k] - best) + biases[k]), axis=0, keepdims=True)
    lane = lax.broadcasted_iota(jnp.int32, (rows, at), 1)
    line = lax.broadcasted_iota(jnp.int32, (rows, at), 0)
    per = 8 * LOOP
    slot = ((lane // per + shift_ref[0]) % RESIDUES) * LOOP + (lane // 8) % LOOP
    mine = slot == line
    query = lax.broadcasted_iota(jnp.int32, (at, 128), 0) % 8
    column = lax.broadcasted_iota(jnp.int32, (at, 128), 1)
    value = lax.dot_general(
        jnp.where(mine, best, 0.0),
        (query == column).astype(jnp.float32),
        (((1,), (0,)), ((), ())),
        precision=lax.Precision.HIGHEST,
        preferred_element_type=jnp.float32,
    ) + lax.dot_general(
        jnp.where(mine, total, 0.0),
        (query + 8 == column).astype(jnp.float32),
        (((1,), (0,)), ((), ())),
        precision=lax.Precision.HIGHEST,
        preferred_element_type=jnp.float32,
    )
    out_ref[:rows, :] = value
    out_ref[rows:, :] = value


def finish_kernel(in_ref, soft_ref, top_ref):
    rows = in_ref.shape[0] // 2
    halves = []
    for side in range(2):
        part = in_ref[side * rows : (side + 1) * rows, :]
        best = jnp.max(part, axis=0, keepdims=True)
        totals = pltpu.roll(part, 120, 1)
        total = jnp.sum(totals * jnp.exp(2.0 * jnp.minimum(part - best, 0.0)), axis=0, keepdims=True)
        halves.append((2.0 * best + jnp.log(total), best))
    first = lax.broadcasted_iota(jnp.int32, (1, 128), 1) < 8
    for out_ref, one, two in zip((soft_ref, top_ref), *halves):
        out_ref[...] = jnp.where(first, one, pltpu.roll(two, 8, 1))[:, :16]


def shards(queries, spans, span_doc, span_valid, doc_bias):
    side = lax.axis_index("merge")
    place = lax.axis_index("ring")
    half = queries.shape[0] // 2
    mine = lax.dynamic_slice_in_dim(queries, side * half, half, 0)
    code = jnp.where(span_valid == 1, span_doc, doc_bias.shape[0]).astype(jnp.bfloat16)
    codes = jnp.pad(code[None, :], ((0, 7), (0, spans.shape[1] - code.shape[0])))
    pack = jnp.concatenate([spans, codes], axis=0)

    loops = [[ring_place(r, i) for i in range(LOOP)] for r in range(RESIDUES)]
    near = lax.all_to_all(
        jnp.broadcast_to(mine[None], (LOOP, *mine.shape)), "ring", 0, 0, axis_index_groups=loops, tiled=True
    )
    row_packs = [pack, shifted(pack, "row", 1), shifted(pack, "row", -1), shifted(pack, "row", 2)]
    packs = row_packs + [shifted(one, "merge", 1) for one in row_packs]
    up = shifted(near, "ring", -1)
    down = shifted(near, "ring", 1)
    far_up = shifted(near[: LOOP // 2], "ring", -2)
    far_down = shifted(near[LOOP // 2 :], "ring", 2)

    slots = RING * 2
    stats = pl.pallas_call(
        scores_kernel,
        out_shape=jax.ShapeDtypeStruct((slots, 128), jnp.float32),
        in_specs=[pl.BlockSpec(memory_space=pltpu.SMEM)] + [pl.BlockSpec(memory_space=pltpu.VMEM)] * 14,
        out_specs=pl.BlockSpec(memory_space=pltpu.VMEM),
        scratch_shapes=[
            pltpu.VMEM((RING * half, spans.shape[1]), jnp.bfloat16),
            pltpu.VMEM((8, spans.shape[0], RING * half), jnp.float32),
        ],
        name="scores",
    )(
        (place % RESIDUES).astype(jnp.int32)[None],
        doc_bias[None, :],
        *packs,
        near,
        up,
        far_up,
        far_down,
        down,
    )
    owners = [
        (ring_place(r, i) * ROW + x) * 2 + m
        for x in range(ROW)
        for m in range(2)
        for r in range(RESIDUES)
        for i in range(LOOP)
    ]
    columns = [owners[k * slots : (k + 1) * slots] for k in range(ROW)]
    got = lax.all_to_all(stats, GROUP, 0, 0, axis_index_groups=columns, tiled=True)
    soft, top = pl.pallas_call(
        finish_kernel,
        out_shape=[jax.ShapeDtypeStruct((1, 2 * half), jnp.float32)] * 2,
        in_specs=[pl.BlockSpec(memory_space=pltpu.VMEM)],
        out_specs=[pl.BlockSpec(memory_space=pltpu.VMEM)] * 2,
        name="finish",
    )(got)
    return soft.reshape(-1), top.reshape(-1)


def solution(mesh):
    split = Mesh(
        mesh.devices.reshape(mesh.shape["parts"], RING, ROW, mesh.shape["merge"]),
        ("parts", *GROUP),
    )
    blk = ("ring", "row")
    every = ("parts", *GROUP)
    owned = P(("parts", *blk))
    return jax.shard_map(
        shards,
        mesh=split,
        in_specs=(P(blk, None), P(every, None), P(every), P(every), P()),
        out_specs=(owned, owned),
        check_vma=False,
    )
```

```python
import jax
import jax.numpy as jnp
from jax import lax
from jax.experimental import pallas as pl
from jax.experimental.pallas import tpu as pltpu
from jax.sharding import Mesh
from jax.sharding import PartitionSpec as P

RING = 32
ROW = 4
RESIDUES = 4
LOOP = RING // RESIDUES
FIRST = RING - RESIDUES
LAST = RING // 2
LOW = -1e30

GROUP = ("ring", "row", "merge")


def ring_place(residue, step, start=FIRST):
    return (start + RESIDUES * step + residue) % RING


def shifted(value, axis, by):
    size = lax.axis_size(axis)
    return lax.ppermute(value, axis, [(k, (k + by) % size) for k in range(size)])


def mirrored(value, mask):
    size = lax.axis_size("row")
    return lax.ppermute(value, "row", [(k, k ^ mask) for k in range(size)])


def in_vmem(value):
    return pltpu.with_memory_space_constraint(value, pltpu.MemorySpace.VMEM)


def scores_kernel(shift_ref, bias_ref, *refs):
    pairs, pieces, out_ref = refs[:4], refs[4:9], refs[9]
    rows_ref, sims_ref = refs[10:]
    packs = [pair.at[k] for pair in pairs for k in range(2)]
    rows = out_ref.shape[0] // 2
    at = 0
    for piece in pieces:
        size = piece.shape[0] * piece.shape[1]
        rows_ref[at : at + size, :] = piece[...].reshape(size, piece.shape[2])
        at += size
    count = packs[0].shape[0] - 8
    docs = lax.broadcasted_iota(jnp.int32, (count, bias_ref.shape[1]), 1).astype(jnp.float32)
    best = jnp.full((1, at), LOW, jnp.float32)
    biases = []
    for k, pack in enumerate(packs):
        code = pack[count:, :128].astype(jnp.float32).T[:, :1]
        bias = jnp.sum(jnp.where(docs == code, bias_ref[...], 0.0), axis=1, keepdims=True)
        valid = code < float(bias_ref.shape[1])
        biases.append(jnp.where(valid, bias, -jnp.inf))
        sim = lax.dot_general(
            pack[:count, :], rows_ref[...], (((1,), (1,)), ((), ())), preferred_element_type=jnp.float32
        )
        sims_ref[k] = sim
        best = jnp.maximum(best, jnp.max(jnp.where(valid, sim, LOW), axis=0, keepdims=True))
    total = jnp.zeros((1, at), jnp.float32)
    for k in range(len(packs)):
        total += jnp.sum(jnp.exp(2.0 * (sims_ref[k] - best) + biases[k]), axis=0, keepdims=True)
    lane = lax.broadcasted_iota(jnp.int32, (rows, at), 1)
    line = lax.broadcasted_iota(jnp.int32, (rows, at), 0)
    per = 8 * LOOP
    turn = (LAST - FIRST) // RESIDUES
    slot = ((lane // per + shift_ref[0]) % RESIDUES) * LOOP + (lane // 8 + LOOP - turn) % LOOP
    mine = slot == line
    query = lax.broadcasted_iota(jnp.int32, (at, 128), 0) % 8
    column = lax.broadcasted_iota(jnp.int32, (at, 128), 1)
    value = lax.dot_general(
        jnp.where(mine, best, 0.0),
        (query == column).astype(jnp.float32),
        (((1,), (0,)), ((), ())),
        precision=lax.Precision.HIGHEST,
        preferred_element_type=jnp.float32,
    ) + lax.dot_general(
        jnp.where(mine, total, 0.0),
        (query + 8 == column).astype(jnp.float32),
        (((1,), (0,)), ((), ())),
        precision=lax.Precision.HIGHEST,
        preferred_element_type=jnp.float32,
    )
    out_ref[:rows, :] = value
    out_ref[rows:, :] = value


def finish_kernel(in_ref, soft_ref, top_ref):
    rows = in_ref.shape[0] // 2
    halves = []
    for side in range(2):
        part = in_ref[side * rows : (side + 1) * rows, :]
        best = jnp.max(part, axis=0, keepdims=True)
        totals = pltpu.roll(part, 120, 1)
        total = jnp.sum(totals * jnp.exp(2.0 * jnp.minimum(part - best, 0.0)), axis=0, keepdims=True)
        halves.append((2.0 * best + jnp.log(total), best))
    first = lax.broadcasted_iota(jnp.int32, (1, 128), 1) < 8
    for out_ref, one, two in zip((soft_ref, top_ref), *halves):
        out_ref[...] = jnp.where(first, one, pltpu.roll(two, 8, 1))[:, :16]


def shards(queries, spans, span_doc, span_valid, doc_bias):
    side = lax.axis_index("merge")
    place = lax.axis_index("ring")
    half = queries.shape[0] // 2
    mine = lax.dynamic_slice_in_dim(queries, side * half, half, 0)
    code = jnp.where(span_valid == 1, span_doc, doc_bias.shape[0]).astype(jnp.bfloat16)
    codes = jnp.pad(code[None, :], ((0, 7), (0, spans.shape[1] - code.shape[0])))
    pack = jnp.concatenate([spans, codes], axis=0)

    loops = [[ring_place(r, i) for i in range(LOOP)] for r in range(RESIDUES)]
    near = lax.all_to_all(
        jnp.broadcast_to(mine[None], (LOOP, *mine.shape)), "ring", 0, 0, axis_index_groups=loops, tiled=True
    )
    two = jnp.stack([pack, mirrored(pack, 1)])
    four = [two, mirrored(two, 3)]
    pairs = four + [shifted(one, "merge", 1) for one in four]
    up = shifted(near, "ring", -1)
    down = shifted(near, "ring", 1)
    far_up = shifted(near[: LOOP // 2], "ring", -2)
    far_down = shifted(near[LOOP // 2 :], "ring", 2)

    slots = RING * 2
    stats = pl.pallas_call(
        scores_kernel,
        out_shape=jax.ShapeDtypeStruct((slots, 128), jnp.float32),
        in_specs=[pl.BlockSpec(memory_space=pltpu.SMEM)] + [pl.BlockSpec(memory_space=pltpu.VMEM)] * 10,
        out_specs=pl.BlockSpec(memory_space=pltpu.VMEM),
        scratch_shapes=[
            pltpu.VMEM((RING * half, spans.shape[1]), jnp.bfloat16),
            pltpu.VMEM((8, spans.shape[0], RING * half), jnp.float32),
        ],
        name="scores",
    )(
        (place % RESIDUES).astype(jnp.int32)[None],
        doc_bias[None, :],
        *[in_vmem(pair) for pair in pairs],
        *[in_vmem(piece) for piece in (near, up, far_up, far_down, down)],
    )
    owners = [
        (ring_place(r, i, LAST) * ROW + x) * 2 + m
        for x in range(ROW)
        for m in range(2)
        for r in range(RESIDUES)
        for i in range(LOOP)
    ]
    columns = [owners[k * slots : (k + 1) * slots] for k in range(ROW)]
    got = lax.all_to_all(stats, GROUP, 0, 0, axis_index_groups=columns, tiled=True)
    soft, top = pl.pallas_call(
        finish_kernel,
        out_shape=[jax.ShapeDtypeStruct((1, 2 * half), jnp.float32)] * 2,
        in_specs=[pl.BlockSpec(memory_space=pltpu.VMEM)],
        out_specs=[pl.BlockSpec(memory_space=pltpu.VMEM)] * 2,
        name="finish",
    )(in_vmem(got))
    return soft.reshape(-1), top.reshape(-1)


def solution(mesh):
    split = Mesh(
        mesh.devices.reshape(mesh.shape["parts"], RING, ROW, mesh.shape["merge"]),
        ("parts", *GROUP),
    )
    blk = ("ring", "row")
    every = ("parts", *GROUP)
    owned = P(("parts", *blk))
    return jax.shard_map(
        shards,
        mesh=split,
        in_specs=(P(blk, None), P(every, None), P(every), P(every), P()),
        out_specs=(owned, owned),
        check_vma=False,
    )
```

```python
import jax
import jax.numpy as jnp
from jax import lax
from jax.experimental import pallas as pl
from jax.experimental.pallas import tpu as pltpu
from jax.sharding import Mesh
from jax.sharding import PartitionSpec as P


RING = 32
ROW = 4
RESIDUES = 4
LOOP = RING // RESIDUES
FIRST = RING - RESIDUES
LAST = RING // 2
LOW = -1e30

GROUP = ("ring", "row", "merge")


def ring_place(residue, step, start=FIRST):
    return (start + RESIDUES * step + residue) % RING


def shifted(value, axis, by):
    size = lax.axis_size(axis)
    return lax.ppermute(value, axis, [(k, (k + by) % size) for k in range(size)])


def mirrored(value, mask):
    size = lax.axis_size("row")
    return lax.ppermute(value, "row", [(k, k ^ mask) for k in range(size)])


def in_vmem(value):
    return pltpu.with_memory_space_constraint(value, pltpu.MemorySpace.VMEM)


def scores_kernel(shift_ref, bias_ref, *refs):
    pairs, pieces, out_ref = refs[:4], refs[4:8], refs[8]
    rows_ref, sims_ref = refs[9:]
    packs = [pair.at[k] for pair in pairs for k in range(2)]
    rows = out_ref.shape[0] // 2
    at = 0
    for piece in pieces:
        size = piece.shape[0] * piece.shape[1]
        rows_ref[at : at + size, :] = piece[...].reshape(size, piece.shape[2])
        at += size
    count = packs[0].shape[0] - 8
    docs = lax.broadcasted_iota(jnp.int32, (count, bias_ref.shape[1]), 1).astype(jnp.float32)
    best = jnp.full((1, at), LOW, jnp.float32)
    biases = []
    for k, pack in enumerate(packs):
        code = pack[count:, :128].astype(jnp.float32).T[:, :1]
        bias = jnp.sum(jnp.where(docs == code, bias_ref[...], 0.0), axis=1, keepdims=True)
        valid = code < float(bias_ref.shape[1])
        biases.append(jnp.where(valid, bias, -jnp.inf))
        sim = lax.dot_general(
            pack[:count, :], rows_ref[...], (((1,), (1,)), ((), ())), preferred_element_type=jnp.float32
        )
        sims_ref[k] = sim
        best = jnp.maximum(best, jnp.max(jnp.where(valid, sim, LOW), axis=0, keepdims=True))
    total = jnp.zeros((1, at), jnp.float32)
    for k in range(len(packs)):
        total += jnp.sum(jnp.exp(2.0 * (sims_ref[k] - best) + biases[k]), axis=0, keepdims=True)
    lane = lax.broadcasted_iota(jnp.int32, (rows, at), 1)
    line = lax.broadcasted_iota(jnp.int32, (rows, at), 0)
    per = 8 * LOOP
    turn = (LAST - FIRST) // RESIDUES
    slot = ((lane // per + shift_ref[0]) % RESIDUES) * LOOP + (lane // 8 + LOOP - turn) % LOOP
    mine = slot == line
    query = lax.broadcasted_iota(jnp.int32, (at, 128), 0) % 8
    column = lax.broadcasted_iota(jnp.int32, (at, 128), 1)
    value = lax.dot_general(
        jnp.where(mine, best, 0.0),
        (query == column).astype(jnp.float32),
        (((1,), (0,)), ((), ())),
        precision=lax.Precision.HIGHEST,
        preferred_element_type=jnp.float32,
    ) + lax.dot_general(
        jnp.where(mine, total, 0.0),
        (query + 8 == column).astype(jnp.float32),
        (((1,), (0,)), ((), ())),
        precision=lax.Precision.HIGHEST,
        preferred_element_type=jnp.float32,
    )
    out_ref[:rows, :] = value
    out_ref[rows:, :] = value


def finish_kernel(in_ref, soft_ref, top_ref):
    rows = in_ref.shape[0] // 2
    halves = []
    for side in range(2):
        part = in_ref[side * rows : (side + 1) * rows, :]
        best = jnp.max(part, axis=0, keepdims=True)
        totals = pltpu.roll(part, 120, 1)
        total = jnp.sum(totals * jnp.exp(2.0 * jnp.minimum(part - best, 0.0)), axis=0, keepdims=True)
        halves.append((2.0 * best + jnp.log(total), best))
    first = lax.broadcasted_iota(jnp.int32, (1, 128), 1) < 8
    for out_ref, one, two in zip((soft_ref, top_ref), *halves):
        out_ref[...] = jnp.where(first, one, pltpu.roll(two, 8, 1))[:, :16]


def shards(queries, spans, span_doc, span_valid, doc_bias):
    side = lax.axis_index("merge")
    place = lax.axis_index("ring")
    half = queries.shape[0] // 2
    mine = lax.dynamic_slice_in_dim(queries, side * half, half, 0)
    code = jnp.where(span_valid == 1, span_doc, doc_bias.shape[0]).astype(jnp.bfloat16)
    codes = jnp.pad(code[None, :], ((0, 7), (0, spans.shape[1] - code.shape[0])))
    pack = jnp.concatenate([spans, codes], axis=0)

    loops = [[ring_place(r, i) for i in range(LOOP)] for r in range(RESIDUES)]
    copies = jnp.broadcast_to(mine[None], (LOOP, *mine.shape))
    near = lax.all_to_all(copies, "ring", 0, 0, axis_index_groups=loops, tiled=True)
    other = mirrored(pack, 1)
    two = jnp.stack([pack, other])
    four = [two, mirrored(two, 3)]
    pairs = four + [shifted(one, "merge", 1) for one in four]
    up = shifted(near, "ring", -1)
    down = shifted(near, "ring", 1)
    across = lax.ppermute(near, "ring", [(k, (k + 4 * (k % 2) - 2) % RING) for k in range(RING)])

    slots = RING * 2
    stats = pl.pallas_call(
        scores_kernel,
        out_shape=jax.ShapeDtypeStruct((slots, 128), jnp.float32),
        in_specs=[pl.BlockSpec(memory_space=pltpu.SMEM)] + [pl.BlockSpec(memory_space=pltpu.VMEM)] * 9,
        out_specs=pl.BlockSpec(memory_space=pltpu.VMEM),
        scratch_shapes=[
            pltpu.VMEM((RING * half, spans.shape[1]), jnp.bfloat16),
            pltpu.VMEM((8, spans.shape[0], RING * half), jnp.float32),
        ],
        name="scores",
    )(
        (place % RESIDUES).astype(jnp.int32)[None],
        doc_bias[None, :],
        *[in_vmem(pair) for pair in pairs],
        *[in_vmem(piece) for piece in (near, up, across, down)],
    )
    owners = [
        (ring_place(r, i, LAST) * ROW + x) * 2 + m
        for x in range(ROW)
        for m in range(2)
        for r in range(RESIDUES)
        for i in range(LOOP)
    ]
    columns = [owners[k * slots : (k + 1) * slots] for k in range(ROW)]
    got = lax.all_to_all(stats, GROUP, 0, 0, axis_index_groups=columns, tiled=True)
    soft, top = pl.pallas_call(
        finish_kernel,
        out_shape=[jax.ShapeDtypeStruct((1, 2 * half), jnp.float32)] * 2,
        in_specs=[pl.BlockSpec(memory_space=pltpu.VMEM)],
        out_specs=[pl.BlockSpec(memory_space=pltpu.VMEM)] * 2,
        name="finish",
    )(in_vmem(got))
    return soft.reshape(-1), top.reshape(-1)


def solution(mesh):
    split = Mesh(
        mesh.devices.reshape(mesh.shape["parts"], RING, ROW, mesh.shape["merge"]),
        ("parts", *GROUP),
    )
    blk = ("ring", "row")
    every = ("parts", *GROUP)
    owned = P(("parts", *blk))
    return jax.shard_map(
        shards,
        mesh=split,
        in_specs=(P(blk, None), P(every, None), P(every), P(every), P()),
        out_specs=(owned, owned),
        check_vma=False,
    )
```

```python
import jax
import jax.numpy as jnp
from jax import lax
from jax.experimental import pallas as pl
from jax.experimental.pallas import tpu as pltpu
from jax.sharding import Mesh
from jax.sharding import PartitionSpec as P


RING = 32
ROW = 4
RESIDUES = 4
LOOP = RING // RESIDUES
FIRST = RING - RESIDUES
LAST = RING // 2
LOW = -1e30

GROUP = ("ring", "row", "merge")


def ring_place(residue, step, start=FIRST):
    return (start + RESIDUES * step + residue) % RING


def shifted(value, axis, by):
    size = lax.axis_size(axis)
    return lax.ppermute(value, axis, [(k, (k + by) % size) for k in range(size)])


def mirrored(value, mask):
    size = lax.axis_size("row")
    return lax.ppermute(value, "row", [(k, k ^ mask) for k in range(size)])


def in_vmem(value):
    return pltpu.with_memory_space_constraint(value, pltpu.MemorySpace.VMEM)


def scores_kernel(shift_ref, bias_ref, *refs):
    pairs, pieces, out_ref = refs[:4], refs[4:8], refs[8]
    rows_ref, sims_ref = refs[9:]
    packs = [pair.at[k] for pair in pairs for k in range(2)]
    rows = out_ref.shape[0] // 2
    at = 0
    for piece in pieces:
        size = piece.shape[0] * piece.shape[1]
        rows_ref[at : at + size, :] = piece[...].reshape(size, piece.shape[2])
        at += size
    count = packs[0].shape[0] - 8
    docs = lax.broadcasted_iota(jnp.int32, (count, bias_ref.shape[1]), 1).astype(jnp.float32)
    whole = jnp.concatenate([pack[:count, :] for pack in packs], axis=0)
    sims_ref[...] = lax.dot_general(
        whole, rows_ref[...], (((1,), (1,)), ((), ())), preferred_element_type=jnp.float32
    ).reshape(sims_ref.shape)
    biases = []
    best = jnp.full((8, at), LOW, jnp.float32)
    for k, pack in enumerate(packs):
        code = pack[count:, :128].astype(jnp.float32).T[:, :1]
        bias = jnp.sum(jnp.where(docs == code, bias_ref[...], 0.0), axis=1, keepdims=True)
        valid = code < float(bias_ref.shape[1])
        biases.append(jnp.where(valid, bias, -jnp.inf))
        sim = jnp.where(valid, sims_ref[k], LOW)
        best = jnp.maximum(best, jnp.max(sim.reshape(count // 8, 8, at), axis=0))
    best = jnp.max(best, axis=0, keepdims=True)
    total = jnp.zeros((8, at), jnp.float32)
    for k in range(len(packs)):
        term = jnp.exp(2.0 * (sims_ref[k] - best) + biases[k])
        total += jnp.sum(term.reshape(count // 8, 8, at), axis=0)
    total = jnp.sum(total, axis=0, keepdims=True)
    lane = lax.broadcasted_iota(jnp.int32, (rows, at), 1)
    line = lax.broadcasted_iota(jnp.int32, (rows, at), 0)
    per = 8 * LOOP
    turn = (LAST - FIRST) // RESIDUES
    slot = ((lane // per + shift_ref[0]) % RESIDUES) * LOOP + (lane // 8 + LOOP - turn) % LOOP
    mine = slot == line
    query = lax.broadcasted_iota(jnp.int32, (at, 128), 0) % 8
    column = lax.broadcasted_iota(jnp.int32, (at, 128), 1)
    value = lax.dot_general(
        jnp.concatenate([jnp.where(mine, best, 0.0), jnp.where(mine, total, 0.0)], axis=1),
        jnp.concatenate([query == column, query + 8 == column], axis=0).astype(jnp.float32),
        (((1,), (0,)), ((), ())),
        precision=lax.Precision.HIGHEST,
        preferred_element_type=jnp.float32,
    )
    out_ref[:rows, :] = value
    out_ref[rows:, :] = value


def finish_kernel(in_ref, soft_ref, top_ref):
    rows = in_ref.shape[0] // 2
    halves = []
    for side in range(2):
        part = in_ref[side * rows : (side + 1) * rows, :]
        best = jnp.max(part, axis=0, keepdims=True)
        totals = pltpu.roll(part, 120, 1)
        total = jnp.sum(totals * jnp.exp(2.0 * jnp.minimum(part - best, 0.0)), axis=0, keepdims=True)
        halves.append((2.0 * best + jnp.log(total), best))
    first = lax.broadcasted_iota(jnp.int32, (1, 128), 1) < 8
    for out_ref, one, two in zip((soft_ref, top_ref), *halves):
        out_ref[...] = jnp.where(first, one, pltpu.roll(two, 8, 1))[:, :16]


def shards(queries, spans, span_doc, span_valid, doc_bias):
    side = lax.axis_index("merge")
    place = lax.axis_index("ring")
    half = queries.shape[0] // 2
    code = jnp.where(span_valid == 1, span_doc, doc_bias.shape[0]).astype(jnp.bfloat16)
    codes = jnp.pad(code[None, :], ((0, 7), (0, spans.shape[1] - code.shape[0])))
    pack = jnp.concatenate([spans, codes], axis=0)

    loops = [[ring_place(r, i) for i in range(LOOP)] for r in range(RESIDUES)]
    mine = lax.dynamic_slice_in_dim(queries, side * half, half, 0)
    copies = jnp.broadcast_to(mine[None], (LOOP, *mine.shape))
    near = lax.all_to_all(copies, "ring", 0, 0, axis_index_groups=loops, tiled=True)
    other = mirrored(pack, 1)
    two = jnp.stack([pack, other])
    four = [two, mirrored(two, 3)]
    pairs = [*four, shifted(two, "merge", 1)]
    pairs.append(shifted(four[1], "merge", 1))
    up = shifted(near, "ring", -1)
    down = shifted(near, "ring", 1)
    across = lax.ppermute(near, "ring", [(k, (k + 4 * (k % 2) - 2) % RING) for k in range(RING)])

    slots = RING * 2
    stats = pl.pallas_call(
        scores_kernel,
        out_shape=pltpu.VMEM((slots, 128), jnp.float32),
        in_specs=[pl.BlockSpec(memory_space=pltpu.SMEM)] + [pl.BlockSpec(memory_space=pltpu.VMEM)] * 9,
        out_specs=pl.BlockSpec(memory_space=pltpu.VMEM),
        scratch_shapes=[
            pltpu.VMEM((RING * half, spans.shape[1]), jnp.bfloat16),
            pltpu.VMEM((8, spans.shape[0], RING * half), jnp.float32),
        ],
        name="scores",
    )(
        (place % RESIDUES).astype(jnp.int32)[None],
        doc_bias[None, :],
        *[in_vmem(pair) for pair in pairs],
        *[in_vmem(piece) for piece in (near, up, across, down)],
    )
    owners = [
        (ring_place(r, i, LAST) * ROW + x) * 2 + m
        for x in range(ROW)
        for m in range(2)
        for r in range(RESIDUES)
        for i in range(LOOP)
    ]
    columns = [owners[k * slots : (k + 1) * slots] for k in range(ROW)]
    got = lax.all_to_all(stats, GROUP, 0, 0, axis_index_groups=columns, tiled=True)
    soft, top = pl.pallas_call(
        finish_kernel,
        out_shape=[jax.ShapeDtypeStruct((1, 2 * half), jnp.float32)] * 2,
        in_specs=[pl.BlockSpec(memory_space=pltpu.VMEM)],
        out_specs=[pl.BlockSpec(memory_space=pltpu.VMEM)] * 2,
        name="finish",
    )(in_vmem(got))
    return soft.reshape(-1), top.reshape(-1)


def solution(mesh):
    split = Mesh(
        mesh.devices.reshape(mesh.shape["parts"], RING, ROW, mesh.shape["merge"]),
        ("parts", *GROUP),
    )
    blk = ("ring", "row")
    every = ("parts", *GROUP)
    owned = P(("parts", *blk))
    return jax.shard_map(
        shards,
        mesh=split,
        in_specs=(P(blk, None), P(every, None), P(every), P(every), P()),
        out_specs=(owned, owned),
        check_vma=False,
    )
```

```python
import jax
import jax.numpy as jnp
from jax import lax
from jax.experimental import pallas as pl
from jax.experimental.pallas import tpu as pltpu
from jax.sharding import Mesh
from jax.sharding import PartitionSpec as P


RING = 32
ROW = 4
RESIDUES = 4
LOOP = RING // RESIDUES
FIRST = RING - 2 * RESIDUES
TURN = 3 * LOOP // 4
LOW = -1e30

GROUP = ("ring", "row", "merge")


def ring_place(residue, step):
    return (FIRST + RESIDUES * step + residue) % RING


def shifted(value, axis, by):
    size = lax.axis_size(axis)
    return lax.ppermute(value, axis, [(k, (k + by) % size) for k in range(size)])


def mirrored(value, mask):
    size = lax.axis_size("row")
    return lax.ppermute(value, "row", [(k, k ^ mask) for k in range(size)])


def in_vmem(value):
    return pltpu.with_memory_space_constraint(value, pltpu.MemorySpace.VMEM)


def scores_kernel(shift_ref, bias_ref, *refs):
    pairs, pieces, out_ref = refs[:4], refs[4:8], refs[8]
    rows_ref, sims_ref = refs[9:]
    packs = [pair.at[k] for pair in pairs for k in range(2)]
    rows = out_ref.shape[0] // 2
    at = 0
    for piece in pieces:
        size = piece.shape[0] * piece.shape[1]
        rows_ref[at : at + size, :] = piece[...].reshape(size, piece.shape[2])
        at += size
    count = packs[0].shape[0] - 8
    docs = lax.broadcasted_iota(jnp.int32, (count, bias_ref.shape[1]), 1).astype(jnp.float32)
    whole = jnp.concatenate([pack[:count, :] for pack in packs], axis=0)
    sims_ref[...] = lax.dot_general(
        whole, rows_ref[...], (((1,), (1,)), ((), ())), preferred_element_type=jnp.float32
    ).reshape(sims_ref.shape)
    biases = []
    best = jnp.full((8, at), LOW, jnp.float32)
    for k, pack in enumerate(packs):
        code = pack[count:, :128].astype(jnp.float32).T[:, :1]
        bias = jnp.sum(jnp.where(docs == code, bias_ref[...], 0.0), axis=1, keepdims=True)
        valid = code < float(bias_ref.shape[1])
        biases.append(jnp.where(valid, bias, -jnp.inf))
        sim = jnp.where(valid, sims_ref[k], LOW)
        best = jnp.maximum(best, jnp.max(sim.reshape(count // 8, 8, at), axis=0))
    best = jnp.max(best, axis=0, keepdims=True)
    total = jnp.zeros((8, at), jnp.float32)
    for k in range(len(packs)):
        term = jnp.exp(2.0 * (sims_ref[k] - best) + biases[k])
        total += jnp.sum(term.reshape(count // 8, 8, at), axis=0)
    total = jnp.sum(total, axis=0, keepdims=True)
    lane = lax.broadcasted_iota(jnp.int32, (rows, at), 1)
    line = lax.broadcasted_iota(jnp.int32, (rows, at), 0)
    per = 8 * LOOP
    slot = ((lane // per + shift_ref[0]) % RESIDUES) * LOOP + (lane // 8 + LOOP - TURN) % LOOP
    mine = slot == line
    query = lax.broadcasted_iota(jnp.int32, (at, 128), 0) % 8
    column = lax.broadcasted_iota(jnp.int32, (at, 128), 1)
    value = lax.dot_general(
        jnp.concatenate([jnp.where(mine, best, 0.0), jnp.where(mine, total, 0.0)], axis=1),
        jnp.concatenate([query == column, query + 8 == column], axis=0).astype(jnp.float32),
        (((1,), (0,)), ((), ())),
        precision=lax.Precision.HIGHEST,
        preferred_element_type=jnp.float32,
    )
    out_ref[:rows, :] = value
    out_ref[rows:, :] = value


def finish_kernel(in_ref, soft_ref, top_ref):
    rows = in_ref.shape[0] // 2
    halves = []
    for side in range(2):
        part = in_ref[side * rows : (side + 1) * rows, :]
        best = jnp.max(part, axis=0, keepdims=True)
        totals = pltpu.roll(part, 120, 1)
        total = jnp.sum(totals * jnp.exp(2.0 * jnp.minimum(part - best, 0.0)), axis=0, keepdims=True)
        halves.append((2.0 * best + jnp.log(total), best))
    first = lax.broadcasted_iota(jnp.int32, (1, 128), 1) < 8
    for out_ref, one, two in zip((soft_ref, top_ref), *halves):
        out_ref[...] = jnp.where(first, one, pltpu.roll(two, 8, 1))[:, :16]


def shards(queries, spans, span_doc, span_valid, doc_bias):
    side = lax.axis_index("merge")
    place = lax.axis_index("ring")
    half = queries.shape[0] // 2
    code = jnp.where(span_valid == 1, span_doc, doc_bias.shape[0]).astype(jnp.bfloat16)
    codes = jnp.pad(code[None, :], ((0, 7), (0, spans.shape[1] - code.shape[0])))
    pack = jnp.concatenate([spans, codes], axis=0)

    loops = [[ring_place(r, i) for i in range(LOOP)] for r in range(RESIDUES)]
    mine = lax.dynamic_slice_in_dim(queries, side * half, half, 0)
    copies = jnp.broadcast_to(mine[None], (LOOP, *mine.shape))
    near = lax.all_to_all(copies, "ring", 0, 0, axis_index_groups=loops, tiled=True)
    other = mirrored(pack, 1)
    two = jnp.stack([pack, other])
    four = [two, mirrored(two, 3)]
    pairs = [*four, shifted(two, "merge", 1)]
    pairs.append(shifted(four[1], "merge", 1))
    across = shifted(near, "ring", 2)
    down = shifted(near, "ring", 1)
    up = shifted(near, "ring", -1)
    slots = RING * 2
    stats = pl.pallas_call(
        scores_kernel,
        out_shape=pltpu.VMEM((slots, 128), jnp.float32),
        in_specs=[pl.BlockSpec(memory_space=pltpu.SMEM)] + [pl.BlockSpec(memory_space=pltpu.VMEM)] * 9,
        out_specs=pl.BlockSpec(memory_space=pltpu.VMEM),
        scratch_shapes=[
            pltpu.VMEM((RING * half, spans.shape[1]), jnp.bfloat16),
            pltpu.VMEM((8, spans.shape[0], RING * half), jnp.float32),
        ],
        name="scores",
    )(
        ((place + RING - FIRST) % RESIDUES).astype(jnp.int32)[None],
        doc_bias[None, :],
        *[in_vmem(pair) for pair in pairs],
        *[in_vmem(piece) for piece in (near, up, across, down)],
    )
    owners = [
        (ring_place(r, i + TURN) * ROW + x) * 2 + m
        for x in range(ROW)
        for m in range(2)
        for r in range(RESIDUES)
        for i in range(LOOP)
    ]
    columns = [owners[k * slots : (k + 1) * slots] for k in range(ROW)]
    got = lax.all_to_all(stats, GROUP, 0, 0, axis_index_groups=columns, tiled=True)
    soft, top = pl.pallas_call(
        finish_kernel,
        out_shape=[jax.ShapeDtypeStruct((1, 2 * half), jnp.float32)] * 2,
        in_specs=[pl.BlockSpec(memory_space=pltpu.VMEM)],
        out_specs=[pl.BlockSpec(memory_space=pltpu.VMEM)] * 2,
        name="finish",
    )(in_vmem(got))
    return soft.reshape(-1), top.reshape(-1)


def solution(mesh):
    split = Mesh(
        mesh.devices.reshape(mesh.shape["parts"], RING, ROW, mesh.shape["merge"]),
        ("parts", *GROUP),
    )
    blk = ("ring", "row")
    every = ("parts", *GROUP)
    owned = P(("parts", *blk))
    return jax.shard_map(
        shards,
        mesh=split,
        in_specs=(P(blk, None), P(every, None), P(every), P(every), P()),
        out_specs=(owned, owned),
        check_vma=False,
    )
```

```python
import jax
import jax.numpy as jnp
from jax import lax
from jax.experimental import pallas as pl
from jax.experimental.pallas import tpu as pltpu
from jax.sharding import Mesh
from jax.sharding import PartitionSpec as P


RING = 32
ROW = 4
RESIDUES = 4
LOOP = RING // RESIDUES
FIRST = RING - 2 * RESIDUES
TURN = 3 * LOOP // 4
LOW = -1e30

GROUP = ("ring", "row", "merge")


def ring_place(residue, step):
    return (FIRST + RESIDUES * step + residue) % RING


def shifted(value, axis, by):
    size = lax.axis_size(axis)
    return lax.ppermute(value, axis, [(k, (k + by) % size) for k in range(size)])


def mirrored(value, mask):
    size = lax.axis_size("row")
    return lax.ppermute(value, "row", [(k, k ^ mask) for k in range(size)])


def in_vmem(value):
    return pltpu.with_memory_space_constraint(value, pltpu.MemorySpace.VMEM)


def scores_kernel(shift_ref, bias_ref, *refs):
    pairs, pieces, out_ref = refs[:4], refs[4:8], refs[8]
    rows_ref, sims_ref = refs[9:]
    packs = [pair.at[k] for pair in pairs for k in range(2)]
    rows = out_ref.shape[0] // 2
    at = 0
    for piece in pieces:
        size = piece.shape[0] * piece.shape[1]
        rows_ref[at : at + size, :] = piece[...].reshape(size, piece.shape[2])
        at += size
    count = packs[0].shape[0] - 8
    docs = lax.broadcasted_iota(jnp.int32, (count, bias_ref.shape[1]), 1).astype(jnp.float32)
    whole = jnp.concatenate([pack[:count, :] for pack in packs], axis=0)
    sims_ref[...] = lax.dot_general(
        whole, rows_ref[...], (((1,), (1,)), ((), ())), preferred_element_type=jnp.float32
    ).reshape(sims_ref.shape)
    codes = jnp.concatenate([pack[count:, :128][:1].astype(jnp.float32) for pack in packs], axis=0).T
    biases = []
    best = jnp.full((8, at), LOW, jnp.float32)
    for k in range(len(packs)):
        code = codes[:, k : k + 1]
        bias = jnp.sum(jnp.where(docs == code, bias_ref[...], 0.0), axis=1, keepdims=True)
        valid = code < float(bias_ref.shape[1])
        biases.append(jnp.where(valid, bias, -jnp.inf))
        sim = sims_ref[k] + jnp.where(valid, 0.0, LOW)
        best = jnp.maximum(best, jnp.max(sim.reshape(count // 8, 8, at), axis=0))
    best = jnp.max(best, axis=0, keepdims=True)
    total = jnp.zeros((8, at), jnp.float32)
    for k in range(len(packs)):
        term = jnp.exp(2.0 * (sims_ref[k] - best) + biases[k])
        total += jnp.sum(term.reshape(count // 8, 8, at), axis=0)
    total = jnp.sum(total, axis=0, keepdims=True)
    lane = lax.broadcasted_iota(jnp.int32, (rows, at), 1)
    line = lax.broadcasted_iota(jnp.int32, (rows, at), 0)
    per = 8 * LOOP
    slot = ((lane // per + shift_ref[0]) % RESIDUES) * LOOP + (lane // 8 + LOOP - TURN) % LOOP
    mine = slot == line
    query = lax.broadcasted_iota(jnp.int32, (at, 128), 0) % 8
    column = lax.broadcasted_iota(jnp.int32, (at, 128), 1)
    value = lax.dot_general(
        jnp.concatenate([jnp.where(mine, best, 0.0), jnp.where(mine, total, 0.0)], axis=1),
        jnp.concatenate([query == column, query + 8 == column], axis=0).astype(jnp.float32),
        (((1,), (0,)), ((), ())),
        precision=lax.Precision.HIGHEST,
        preferred_element_type=jnp.float32,
    )
    out_ref[:rows, :] = value
    out_ref[rows:, :] = value


def finish_kernel(in_ref, soft_ref, top_ref):
    rows = in_ref.shape[0] // 2
    halves = []
    for side in range(2):
        part = in_ref[side * rows : (side + 1) * rows, :]
        best = jnp.max(part, axis=0, keepdims=True)
        totals = pltpu.roll(part, 120, 1)
        total = jnp.sum(totals * jnp.exp(2.0 * jnp.minimum(part - best, 0.0)), axis=0, keepdims=True)
        halves.append((2.0 * best + jnp.log(total), best))
    first = lax.broadcasted_iota(jnp.int32, (1, 128), 1) < 8
    for out_ref, one, two in zip((soft_ref, top_ref), *halves):
        out_ref[...] = jnp.where(first, one, pltpu.roll(two, 8, 1))[:, :16]


def shards(queries, spans, span_doc, span_valid, doc_bias):
    side = lax.axis_index("merge")
    place = lax.axis_index("ring")
    half = queries.shape[0] // 2
    code = jnp.where(span_valid == 1, span_doc, doc_bias.shape[0]).astype(jnp.bfloat16)
    codes = jnp.pad(code[None, :], ((0, 7), (0, spans.shape[1] - code.shape[0])))
    pack = jnp.concatenate([spans, codes], axis=0)

    loops = [[ring_place(r, i) for i in range(LOOP)] for r in range(RESIDUES)]
    mine = lax.dynamic_slice_in_dim(queries, side * half, half, 0)
    copies = jnp.broadcast_to(mine[None], (LOOP, *mine.shape))
    near = lax.all_to_all(copies, "ring", 0, 0, axis_index_groups=loops, tiled=True)
    other = mirrored(pack, 1)
    two = jnp.stack([pack, other])
    four = [two, mirrored(two, 3)]
    pairs = [*four, shifted(two, "merge", 1)]
    pairs.append(shifted(four[1], "merge", 1))
    across = shifted(near, "ring", 2)
    down = shifted(near, "ring", 1)
    up = shifted(near, "ring", -1)
    slots = RING * 2
    stats = pl.pallas_call(
        scores_kernel,
        out_shape=pltpu.VMEM((slots, 128), jnp.float32),
        in_specs=[pl.BlockSpec(memory_space=pltpu.SMEM)] + [pl.BlockSpec(memory_space=pltpu.VMEM)] * 9,
        out_specs=pl.BlockSpec(memory_space=pltpu.VMEM),
        scratch_shapes=[
            pltpu.VMEM((RING * half, spans.shape[1]), jnp.bfloat16),
            pltpu.VMEM((8, spans.shape[0], RING * half), jnp.float32),
        ],
        name="scores",
    )(
        ((place + RING - FIRST) % RESIDUES).astype(jnp.int32)[None],
        doc_bias[None, :],
        *[in_vmem(pair) for pair in pairs],
        *[in_vmem(piece) for piece in (near, up, across, down)],
    )
    owners = [
        (ring_place(r, i + TURN) * ROW + x) * 2 + m
        for x in range(ROW)
        for m in range(2)
        for r in range(RESIDUES)
        for i in range(LOOP)
    ]
    columns = [owners[k * slots : (k + 1) * slots] for k in range(ROW)]
    got = lax.all_to_all(stats, GROUP, 0, 0, axis_index_groups=columns, tiled=True)
    soft, top = pl.pallas_call(
        finish_kernel,
        out_shape=[jax.ShapeDtypeStruct((1, 2 * half), jnp.float32)] * 2,
        in_specs=[pl.BlockSpec(memory_space=pltpu.VMEM)],
        out_specs=[pl.BlockSpec(memory_space=pltpu.VMEM)] * 2,
        name="finish",
    )(in_vmem(got))
    return soft.reshape(-1), top.reshape(-1)


def solution(mesh):
    split = Mesh(
        mesh.devices.reshape(mesh.shape["parts"], RING, ROW, mesh.shape["merge"]),
        ("parts", *GROUP),
    )
    blk = ("ring", "row")
    every = ("parts", *GROUP)
    owned = P(("parts", *blk))
    return jax.shard_map(
        shards,
        mesh=split,
        in_specs=(P(blk, None), P(every, None), P(every), P(every), P()),
        out_specs=(owned, owned),
        check_vma=False,
    )
```
